256 devices in a mesh: row: 16 (over x, y), col: 16 (over z, core).
Axes of the slice: x: 4, y: 4, z: 8, core: 2. Of those that a mesh axis runs over, the one named last changes fastest.
Arguments:
- right_side: bfloat16 [16, 16, 8, 128, 256], P('row', 'col'), may hold values from -6 to 6
- diag_inverse: bfloat16 [16, 16, 8, 128, 128], P('row', 'col'), may hold values from -0.5 to 0.5
- panels: bfloat16 [7, 16, 800, 128, 128], P(None, 'row', 'col'), may hold values from -0.0546875 to 0.0546875
- tile_source: int32 [7, 16, 800], P(None, 'row', 'col'), may hold values from 0 to 15
- tile_target: int32 [7, 16, 800], P(None, 'row', 'col'), may hold values from 0 to 15
Outputs:
- solution: float32 [16, 16, 8, 128, 256], P('row', 'col')
The draws below stay inside these ranges and needn't reach their ends.
All inputs are finite; a program needn't handle non-finite values.
Results may differ from the reference program's by a relative error of at most 0.017.
Values may be sent and summed in bfloat16 or wider, within the bound.
A program may use at most 128 MiB of HBM per device.

```python
import jax
import jax.numpy as jnp
from jax import lax

BLOCK = 128
SECTIONS = 8
TPD = 50
COLS = 256
N_ROW = 16
N_COL = 16


def plant(result, rng, least, high):
    place = [jax.random.randint(jax.random.fold_in(rng, axis), (), 0, length) for axis, length in enumerate(result.shape)]
    widest = result.shape.index(max(result.shape))
    beside = place[:widest] + [(place[widest] + 1) % result.shape[widest]] + place[widest + 1:]
    return result.at[tuple(place)].set(least).at[tuple(beside)].set(high)


def block_levels(key, extent, split, smallest, largest):
    loudness = 1.0
    for axis_at, parts in split:
        steps = jax.random.uniform(jax.random.fold_in(jax.random.fold_in(key, 6), axis_at), (parts,), jnp.float32, smallest / len(split), largest / len(split))
        loudness = loudness * jnp.repeat(jnp.exp(steps), extent[axis_at] // parts).reshape((-1,) + (1,) * (len(extent) - 1 - axis_at))
    return loudness


def scatter_about(own_key, extent, deviation, reach, pieces=(), kind=jnp.bfloat16):
    factor_of = block_levels(own_key, extent, pieces, -0.22, 0.18) if pieces else 1.0
    array = jax.random.normal(own_key, extent, jnp.float32) * deviation * factor_of
    return jnp.minimum(jnp.maximum(array, -reach), reach).astype(kind)


def setup_inputs(seed: int = 0) -> dict:
    seeds = jax.random.split(jax.random.key(seed), 6)
    right_side = scatter_about(seeds[0], (N_ROW, N_COL, SECTIONS, BLOCK, COLS), 1.0, 6.0, ((0, 16), (1, 16)))
    diag_inverse = scatter_about(seeds[1], (N_ROW, N_COL, SECTIONS, BLOCK, BLOCK), BLOCK ** -0.5, 0.5, ((0, 16), (1, 16)))
    panels = scatter_about(seeds[2], (SECTIONS - 1, N_ROW, N_COL * TPD, BLOCK, BLOCK), (2 * BLOCK * TPD) ** -0.5, 0.0546875, ((1, 16), (2, 16)))
    tile_source = plant(jax.random.randint(seeds[3], (SECTIONS - 1, N_ROW, N_COL * TPD), 0, N_ROW), jax.random.fold_in(seeds[3], 1), 0, N_ROW - 1).astype(jnp.int32)
    tile_target = plant(jax.random.randint(seeds[4], (SECTIONS - 1, N_ROW, N_COL * TPD), 0, N_COL), jax.random.fold_in(seeds[4], 1), 0, N_COL - 1).astype(jnp.int32)
    return dict(right_side=right_side, diag_inverse=diag_inverse, panels=panels, tile_source=tile_source, tile_target=tile_target)


def round_trip(values):
    low = lax.optimization_barrier(values.astype(jnp.bfloat16))
    return low.astype(jnp.float32)


def reference(right_side, diag_inverse, panels, tile_source, tile_target):
    solved = []
    incoming = jnp.zeros((N_ROW, N_COL, BLOCK, COLS), jnp.float32)
    for section in range(SECTIONS):
        current = right_side[:, :, section].astype(jnp.float32)
        if section > 0:
            current = current - incoming
        current = round_trip(current)
        block = jnp.einsum("ijab,ijbc->ijac", diag_inverse[:, :, section].astype(jnp.float32), current,
                           precision=lax.Precision.HIGHEST)
        solved.append(block)
        if section + 1 < SECTIONS:
            segment = round_trip(block)

            def row_update(items):
                panel_row, source_row, target_row = items
                column_of = (jnp.arange(N_COL * TPD, dtype=jnp.int32) // TPD).astype(jnp.int32)
                picked = segment[source_row, column_of]
                prods = jnp.einsum("qab,qbc->qac", panel_row.astype(jnp.float32), picked,
                                   precision=lax.Precision.HIGHEST)
                prods = prods.reshape(N_COL, TPD, BLOCK * COLS)
                targets = target_row.reshape(N_COL, TPD)
                onehot = (targets[:, None, :] == jnp.arange(N_COL, dtype=jnp.int32)[None, :, None]).astype(jnp.float32)
                shard_sums = jnp.einsum("jtq,jqe->jte", onehot, prods, precision=lax.Precision.HIGHEST)
                shard_sums = round_trip(shard_sums)
                return jnp.sum(shard_sums, axis=0).reshape(N_COL, BLOCK, COLS)

            incoming = lax.map(row_update, (panels[section], tile_source[section], tile_target[section]))
    return jnp.stack(solved, axis=2)
```

```python
import functools
import math

import jax
import jax.numpy as jnp
from jax import lax
from jax.experimental import pallas as pl
from jax.experimental.pallas import tpu as pltpu
from jax.sharding import PartitionSpec as P

MESH = pl.DeviceIdType.MESH
CORES = 2
CHUNKS = 4
VMEM_LIMIT = 60 * 1024 * 1024


def pair_slots(tiles, columns):
    return (tiles + columns) // 2


def tile_tables(source, target, rows, columns):
    levels, tiles = target.shape
    pairs = pair_slots(tiles, columns)
    tile_ids = jnp.arange(tiles, dtype=jnp.int32)
    target_ids = jnp.arange(columns, dtype=jnp.int32)
    hits = (target[:, :, None] == target_ids).astype(jnp.int32)
    count = hits.sum(axis=1)
    need = (count + 1) // 2
    base = jnp.where(target_ids[:, None] < target_ids[None, :], need[:, :, None], 0).sum(axis=1)
    earlier = (target[:, None, :] == target[:, :, None]) & (tile_ids[None, :] < tile_ids[:, None])
    place = 2 * (hits * base[:, None, :]).sum(axis=2) + earlier.astype(jnp.int32).sum(axis=2)
    filled = (place[:, None, :] == jnp.arange(2 * pairs, dtype=jnp.int32)[:, None]).astype(jnp.int32)
    slot_tile = (filled * tile_ids).sum(axis=2)
    slot_source = (filled * (source[:, None, :] - rows)).sum(axis=2) + rows
    opens = (base[:, None, :] == jnp.arange(pairs, dtype=jnp.int32)[:, None]) & (need[:, None, :] > 0)
    keep = 1 - opens.astype(jnp.int32).max(axis=2)
    last = jnp.where(need > 0, base + need - 1, pairs)
    return jnp.concatenate([slot_tile, slot_source, keep, last], axis=1)


def torus_order(rows):
    side = math.isqrt(rows)
    steps = [(dx, dy) for dx in range(side) for dy in range(side) if dx or dy]

    def far(step):
        return -sum(min(part, side - part) for part in step)

    return side, sorted(steps, key=far)


def ring_order(length):
    return sorted(range(1, length), key=lambda step: -min(step, length - step))


def kernel(
    rows, columns, levels, chunks, pairs,
    table, rhs_hbm, diag_hbm, panels_hbm, out,
    rhs, diag, panels, gathered, given, kept, traded, passed, arrived, work, runs, current,
    load_sem, panel_sem, gather_send, gather_recv, trade_send, trade_recv, pass_send, pass_recv,
):
    me_row, me_col = lax.axis_index("row"), lax.axis_index("col")
    floors = columns // CORES
    floor, core = me_col // CORES, lax.rem(me_col, CORES)
    side, row_steps = torus_order(rows)
    me_x, me_y = me_row // side, lax.rem(me_row, side)
    moves = (levels - 1) * chunks
    slots = 2 * pairs
    width = rhs.shape[1]

    def row_peer(step):
        return lax.rem(me_x + step[0], side) * side + lax.rem(me_y + step[1], side)

    def floor_peer(step):
        return lax.rem(floor + step, floors)

    partner = floor * CORES + 1 - core

    loads = [
        pltpu.make_async_copy(rhs_hbm, rhs, load_sem.at[0]),
        pltpu.make_async_copy(diag_hbm, diag, load_sem.at[1]),
    ]
    panel_loads = [
        pltpu.make_async_copy(panels_hbm.at[level], panels.at[level], panel_sem.at[level])
        for level in range(levels - 1)
    ]
    for load in loads + panel_loads:
        load.start()

    barrier = pltpu.get_barrier_semaphore()
    for step in row_steps:
        pl.semaphore_signal(barrier, inc=1, device_id=(row_peer(step), me_col), device_id_type=MESH)
    for step in ring_order(floors):
        pl.semaphore_signal(
            barrier, inc=1, device_id=(me_row, floor_peer(step) * CORES + core), device_id_type=MESH
        )
    pl.semaphore_signal(barrier, inc=1, device_id=(me_row, partner), device_id_type=MESH)

    work[rows] = jnp.zeros_like(work[rows])
    runs[pairs] = jnp.zeros_like(runs[pairs])
    for load in loads:
        load.wait()
    pl.semaphore_wait(barrier, rows - 1 + floors - 1 + 1)

    def landed(ref, sem):
        pltpu.make_async_copy(ref, ref, sem).wait()

    def solve(g):
        level = g // chunks
        current[...] = rhs[g].astype(jnp.float32)

        @pl.when(g >= chunks)
        def _():
            h = g - chunks
            landed(arrived.at[h, pl.ds(0, floors - 1)], pass_recv.at[h])
            incoming = arrived[h, 0].astype(jnp.float32)
            for z in range(1, floors):
                incoming = incoming + arrived[h, z].astype(jnp.float32)
            current[...] = current[...] - incoming

        block = lax.dot_general(
            current[...].astype(jnp.bfloat16), diag[level],
            (((1,), (1,)), ((), ())), preferred_element_type=jnp.float32,
        )

        @pl.when(g < moves)
        def _():
            gathered[g, me_row] = block.astype(jnp.bfloat16)
            for step in row_steps:
                pltpu.make_async_remote_copy(
                    src_ref=gathered.at[g, me_row],
                    dst_ref=gathered.at[g, me_row],
                    send_sem=gather_send.at[g],
                    recv_sem=gather_recv.at[g],
                    device_id=(row_peer(step), me_col),
                    device_id_type=MESH,
                ).start()

        out[g] = block

    def multiply(h):
        level = h // chunks

        @pl.when(h == 0)
        def _():
            for load in panel_loads:
                load.wait()

        landed(gathered.at[h, pl.ds(0, rows - 1)], gather_recv.at[h])
        for row in range(rows):
            work[row] = gathered[h, row]
        total = jnp.zeros((width, rhs.shape[2]), jnp.float32)
        for pair in range(pairs):
            first, second = 2 * pair, 2 * pair + 1
            picked = jnp.concatenate(
                [work[table[level, slots + first]], work[table[level, slots + second]]], axis=1
            )
            tile = jnp.concatenate(
                [panels[level, table[level, first]], panels[level, table[level, second]]], axis=1
            )
            product = lax.dot_general(
                picked, tile, (((1,), (1,)), ((), ())), preferred_element_type=jnp.float32
            )
            total = product + jnp.where(table[level, 2 * slots + pair] != 0, total, 0.0)
            runs[pair] = total.astype(jnp.bfloat16)
        lasts = 2 * slots + pairs
        for z in range(floors):
            given[h, z] = runs[table[level, lasts + CORES * z + 1 - core]]
        pltpu.make_async_remote_copy(
            src_ref=given.at[h],
            dst_ref=traded.at[h],
            send_sem=trade_send.at[h],
            recv_sem=trade_recv.at[h],
            device_id=(me_row, partner),
            device_id_type=MESH,
        ).start()
        for z in range(floors):
            kept[h, z] = runs[table[level, lasts + CORES * z + core]]

    def exchange(h):
        landed(traded.at[h], trade_recv.at[h])

        def both(z):
            return (kept[h, z].astype(jnp.float32) + traded[h, z].astype(jnp.float32)).astype(jnp.bfloat16)

        for step in ring_order(floors):
            z = floor_peer(step)
            passed[h, z] = both(z)
            pltpu.make_async_remote_copy(
                src_ref=passed.at[h, z],
                dst_ref=arrived.at[h, floor],
                send_sem=pass_send.at[h],
                recv_sem=pass_recv.at[h],
                device_id=(me_row, z * CORES + core),
                device_id_type=MESH,
            ).start()
        arrived[h, floor] = both(floor)

    late_product = 1 if chunks >= 4 else 0
    late_exchange = 2 if chunks >= 4 else min(1, chunks - 1)

    def stage(run, h):
        @pl.when((h >= 0) & (h < moves))
        def _():
            run(h)

    def turn(g, carry):
        solve(g)
        if late_product == late_exchange:
            stage(multiply, g - late_product)
            stage(exchange, g - late_exchange)
        else:
            stage(exchange, g - late_exchange)
            stage(multiply, g - late_product)
        return carry

    lax.fori_loop(0, levels * chunks, turn, 0)

    def drain(h, carry):
        landed(gathered.at[h, pl.ds(0, rows - 1)], gather_send.at[h])
        landed(given.at[h], trade_send.at[h])
        landed(passed.at[h, pl.ds(0, floors - 1)], pass_send.at[h])
        return carry

    lax.fori_loop(0, moves, drain, 0)


def local(rows, columns, right_side, diag_inverse, panels, tile_source, tile_target):
    levels, depth, cols = right_side.shape[2:]
    tiles = panels.shape[2]
    chunks = CHUNKS
    width = cols // chunks
    pairs = pair_slots(tiles, columns)
    moves = (levels - 1) * chunks
    floors = columns // CORES
    table = tile_tables(tile_source[:, 0], tile_target[:, 0], rows, columns)
    rhs = jnp.swapaxes(right_side[0, 0], 1, 2).reshape(levels * chunks, width, depth)
    dma = pltpu.SemaphoreType.DMA
    anywhere = pl.BlockSpec(memory_space=pl.ANY)
    solved = pl.pallas_call(
        functools.partial(kernel, rows, columns, levels, chunks, pairs),
        out_shape=jax.ShapeDtypeStruct((levels * chunks, width, depth), jnp.float32),
        in_specs=[pl.BlockSpec(memory_space=pltpu.SMEM), anywhere, anywhere, anywhere],
        out_specs=pl.BlockSpec(memory_space=pltpu.VMEM),
        scratch_shapes=[
            pltpu.VMEM((levels * chunks, width, depth), jnp.bfloat16),
            pltpu.VMEM((levels, depth, depth), jnp.bfloat16),
            pltpu.VMEM((levels - 1, tiles, depth, depth), jnp.bfloat16),
            pltpu.VMEM((moves, rows, width, depth), jnp.bfloat16),
            pltpu.VMEM((moves, floors, width, depth), jnp.bfloat16),
            pltpu.VMEM((moves, floors, width, depth), jnp.bfloat16),
            pltpu.VMEM((moves, floors, width, depth), jnp.bfloat16),
            pltpu.VMEM((moves, floors, width, depth), jnp.bfloat16),
            pltpu.VMEM((moves, floors, width, depth), jnp.bfloat16),
            pltpu.VMEM((rows + 1, width, depth), jnp.bfloat16),
            pltpu.VMEM((pairs + 1, width, depth), jnp.bfloat16),
            pltpu.VMEM((width, depth), jnp.float32),
            dma((2,)),
            dma((levels - 1,)),
            dma((moves,)),
            dma((moves,)),
            dma((moves,)),
            dma((moves,)),
            dma((moves,)),
            dma((moves,)),
        ],
        compiler_params=pltpu.CompilerParams(
            collective_id=0, has_side_effects=True, vmem_limit_bytes=VMEM_LIMIT
        ),
        name="level_solve",
    )(table, rhs, diag_inverse[0, 0], panels[:, 0])
    solved = jnp.swapaxes(solved.reshape(levels, cols, depth), 1, 2)
    return solved[None, None]


def solution(mesh):
    return jax.shard_map(
        functools.partial(local, mesh.shape["row"], mesh.shape["col"]),
        mesh=mesh,
        in_specs=(
            P("row", "col", None, None, None),
            P("row", "col", None, None, None),
            P(None, "row", "col", None, None),
            P(None, "row", "col"),
            P(None, "row", "col"),
        ),
        out_specs=P("row", "col", None, None, None),
        check_vma=False,
    )
```

```python
import functools
import math

import jax
import jax.numpy as jnp
from jax import lax
from jax.experimental import pallas as pl
from jax.experimental.pallas import tpu as pltpu
from jax.sharding import PartitionSpec as P

MESH = pl.DeviceIdType.MESH
CORES = 2
CHUNKS = 8
LISTS = 4
LATE_PRODUCT = 3
LATE_EXCHANGE = 4
NT = (((1,), (1,)), ((), ()))
VMEM_LIMIT = 60 * 1024 * 1024


def ordered_tiles(source, target, rows, columns, tiles):
    lanes = source.shape[1]
    key = (target * lanes + lax.broadcasted_iota(jnp.int32, source.shape, 1)) * rows + source
    across = jnp.broadcast_to(key, (lanes, lanes))
    down = across.T
    place = jnp.sum((down < across).astype(jnp.int32), axis=0, keepdims=True)
    slot = lax.broadcasted_iota(jnp.int32, (lanes, lanes), 1)
    placed = jnp.broadcast_to(place, (lanes, lanes)).T == slot
    ordered = jnp.sum(jnp.where(placed, down, 0), axis=0, keepdims=True)
    ends = jnp.sum((down < (slot + 1) * (lanes * rows)).astype(jnp.int32), axis=0, keepdims=True)
    number = ordered // rows
    return [
        jnp.clip(lax.rem(number, lanes), 0, tiles - 1),
        jnp.clip(lax.rem(ordered, rows), 0, rows - 1),
        number // lanes,
        jnp.clip(ends, 0, tiles),
    ]


def torus_order(rows):
    side = math.isqrt(rows)
    steps = [(dx, dy) for dx in range(side) for dy in range(side) if dx or dy]

    def far(step):
        return -sum(min(part, side - part) for part in step)

    return side, sorted(steps, key=far)


def ring_order(length):
    return sorted(range(1, length), key=lambda step: -min(step, length - step))


def kernel(
    rows, columns, levels, chunks, tiles,
    source_ids, target_ids, rhs_hbm, diag_hbm, panels_hbm, out,
    table, lists, source_pad, target_pad, right, rhs, diag, panels, gathered, given, kept, traded, passed, arrived, work, runs, current,
    load_sem, table_sem, panel_sem, gather_send, gather_recv, trade_send, trade_recv, pass_send, pass_recv,
):
    me_row, me_col = lax.axis_index("row"), lax.axis_index("col")
    floors = columns // CORES
    floor, core = me_col // CORES, lax.rem(me_col, CORES)
    side, row_steps = torus_order(rows)
    me_x, me_y = me_row // side, lax.rem(me_row, side)
    moves = (levels - 1) * chunks
    width, depth = rhs.shape[1:]

    def row_peer(step):
        return lax.rem(me_x + step[0], side) * side + lax.rem(me_y + step[1], side)

    def floor_peer(step):
        return lax.rem(floor + step, floors)

    partner = floor * CORES + 1 - core

    loads = [
        pltpu.make_async_copy(rhs_hbm, right, load_sem.at[0]),
        pltpu.make_async_copy(diag_hbm, diag, load_sem.at[1]),
    ]
    panel_loads = [
        pltpu.make_async_copy(panels_hbm.at[level], panels.at[level], panel_sem.at[level])
        for level in range(levels - 1)
    ]
    for load in loads + panel_loads:
        load.start()

    barrier = pltpu.get_barrier_semaphore()
    for step in row_steps:
        pl.semaphore_signal(barrier, inc=1, device_id=(row_peer(step), me_col), device_id_type=MESH)
    for step in ring_order(floors):
        pl.semaphore_signal(
            barrier, inc=1, device_id=(me_row, floor_peer(step) * CORES + core), device_id_type=MESH
        )
    pl.semaphore_signal(barrier, inc=1, device_id=(me_row, partner), device_id_type=MESH)

    work[rows] = jnp.zeros_like(work[rows])
    runs[tiles] = jnp.zeros_like(runs[tiles])
    for load in loads:
        load.wait()
    with jax.named_scope("wait_barrier"):
        pl.semaphore_wait(barrier, rows - 1 + floors - 1 + 1)

    def turned(level):
        block = right[level].astype(jnp.float32).T
        rhs[pl.ds(level * chunks, chunks)] = block.reshape(chunks, width, depth)

    def plan():
        target_pad[...] = jnp.full_like(target_pad, columns)
        source_pad[...] = jnp.zeros_like(source_pad)
        target_pad[pl.ds(0, levels - 1), pl.ds(0, tiles)] = target_ids[...]
        source_pad[pl.ds(0, levels - 1), pl.ds(0, tiles)] = source_ids[...]
        for level in range(levels - 1):
            found = ordered_tiles(
                source_pad[pl.ds(level, 1)], target_pad[pl.ds(level, 1)], rows, columns, tiles
            )
            for place, values in enumerate(found):
                lists[pl.ds(LISTS * level + place, 1)] = values
        copy = pltpu.make_async_copy(lists, table, table_sem.at[0])
        copy.start()
        for level in range(1, levels):
            turned(level)
        copy.wait()

    def landed(ref, sem):
        pltpu.make_async_copy(ref, ref, sem).wait()

    def solve(g):
        level = g // chunks
        current[...] = rhs[g]

        @pl.when(g >= chunks)
        def _():
            h = g - chunks
            with jax.named_scope("wait_pass"):
                landed(arrived.at[h, pl.ds(0, floors - 1)], pass_recv.at[h])
            incoming = arrived[h, 0].astype(jnp.float32)
            for z in range(1, floors):
                incoming = incoming + arrived[h, z].astype(jnp.float32)
            current[...] = current[...] - incoming

        block = lax.dot_general(
            current[...].astype(jnp.bfloat16), diag[level],
            NT, preferred_element_type=jnp.float32,
        )

        @pl.when(g < moves)
        def _():
            gathered[g, me_row] = block.astype(jnp.bfloat16)
            for step in row_steps:
                pltpu.make_async_remote_copy(
                    src_ref=gathered.at[g, me_row],
                    dst_ref=gathered.at[g, me_row],
                    send_sem=gather_send.at[g],
                    recv_sem=gather_recv.at[g],
                    device_id=(row_peer(step), me_col),
                    device_id_type=MESH,
                ).start()

        out[g] = block

    def multiply(h):
        level = h // chunks

        @pl.when(h == 0)
        def _():
            for load in panel_loads:
                load.wait()

        with jax.named_scope("wait_gather"):
            landed(gathered.at[h, pl.ds(0, rows - 1)], gather_recv.at[h])
        for row in range(rows):
            work[row] = gathered[h, row]
        nothing = jnp.zeros((width, depth), jnp.bfloat16)
        total = jnp.zeros((width, depth), jnp.float32)
        before = -1
        for first in range(0, tiles, 2):
            second = first + 1
            tile = panels[level, table[LISTS * level, first]]
            block = work[table[LISTS * level + 1, first]]
            target = table[LISTS * level + 2, first]
            if second == tiles:
                product = lax.dot_general(block, tile, NT, preferred_element_type=jnp.float32)
                runs[first] = (product + jnp.where(target == before, total, 0.0)).astype(jnp.bfloat16)
                break
            tile = jnp.concatenate([tile, panels[level, table[LISTS * level, second]]], axis=1)
            source = table[LISTS * level + 1, second]
            same = table[LISTS * level + 2, second] == target
            picked = jnp.concatenate(
                [
                    jnp.concatenate([block, work[jnp.where(same, source, rows)]], axis=1),
                    jnp.concatenate([nothing, work[jnp.where(same, rows, source)]], axis=1),
                ],
                axis=0,
            )
            product = lax.dot_general(picked, tile, NT, preferred_element_type=jnp.float32)
            total = product[:width] + jnp.where(target == before, total, 0.0)
            runs[first] = total.astype(jnp.bfloat16)
            total = jnp.where(same, total, product[width:])
            runs[second] = total.astype(jnp.bfloat16)
            before = table[LISTS * level + 2, second]

        def summed(column):
            end = table[LISTS * level + 3, column]
            start = jnp.where(column == 0, 0, table[LISTS * level + 3, jnp.maximum(column - 1, 0)])
            return runs[jnp.where(end > start, end - 1, tiles)]

        for z in range(floors):
            given[h, z] = summed(CORES * z + 1 - core)
        pltpu.make_async_remote_copy(
            src_ref=given.at[h],
            dst_ref=traded.at[h],
            send_sem=trade_send.at[h],
            recv_sem=trade_recv.at[h],
            device_id=(me_row, partner),
            device_id_type=MESH,
        ).start()
        for z in range(floors):
            kept[h, z] = summed(CORES * z + core)

    def exchange(h):
        with jax.named_scope("wait_trade"):
            landed(traded.at[h], trade_recv.at[h])

        def both(z):
            return (kept[h, z].astype(jnp.float32) + traded[h, z].astype(jnp.float32)).astype(jnp.bfloat16)

        for step in ring_order(floors):
            z = floor_peer(step)
            passed[h, z] = both(z)
            pltpu.make_async_remote_copy(
                src_ref=passed.at[h, z],
                dst_ref=arrived.at[h, floor],
                send_sem=pass_send.at[h],
                recv_sem=pass_recv.at[h],
                device_id=(me_row, z * CORES + core),
                device_id_type=MESH,
            ).start()
        arrived[h, floor] = both(floor)

    def stage(run, h):
        @pl.when((h >= 0) & (h < moves))
        def _():
            with jax.named_scope(run.__name__):
                run(h)

    def turn(g, carry):
        @pl.when(g >= chunks)
        def _():
            with jax.named_scope("solve"):
                solve(g)

        stage(multiply, g - LATE_PRODUCT)
        stage(exchange, g - LATE_EXCHANGE)
        return carry

    def begin(g, carry):
        solve(g)
        return carry

    turned(0)
    lax.fori_loop(0, chunks, begin, 0)
    with jax.named_scope("plan"):
        plan()
    lax.fori_loop(0, levels * chunks, turn, 0)

    def drain(h, carry):
        landed(gathered.at[h, pl.ds(0, rows - 1)], gather_send.at[h])
        landed(given.at[h], trade_send.at[h])
        landed(passed.at[h, pl.ds(0, floors - 1)], pass_send.at[h])
        return carry

    lax.fori_loop(0, moves, drain, 0)


def local(rows, columns, right_side, diag_inverse, panels, tile_source, tile_target):
    levels, depth, cols = right_side.shape[2:]
    tiles = panels.shape[2]
    chunks = CHUNKS
    width = cols // chunks
    moves = (levels - 1) * chunks
    floors = columns // CORES
    lanes = -(-tiles // depth) * depth
    dma = pltpu.SemaphoreType.DMA
    anywhere = pl.BlockSpec(memory_space=pl.ANY)
    solved = pl.pallas_call(
        functools.partial(kernel, rows, columns, levels, chunks, tiles),
        out_shape=jax.ShapeDtypeStruct((levels * chunks, width, depth), jnp.float32),
        in_specs=[pl.BlockSpec(memory_space=pltpu.VMEM)] * 2 + [anywhere] * 3,
        out_specs=pl.BlockSpec(memory_space=pltpu.VMEM),
        scratch_shapes=[
            pltpu.SMEM((LISTS * levels, lanes), jnp.int32),
            pltpu.VMEM((LISTS * levels, lanes), jnp.int32),
            pltpu.VMEM((levels, lanes), jnp.int32),
            pltpu.VMEM((levels, lanes), jnp.int32),
            pltpu.VMEM((levels, depth, cols), jnp.bfloat16),
            pltpu.VMEM((levels * chunks, width, depth), jnp.float32),
            pltpu.VMEM((levels, depth, depth), jnp.bfloat16),
            pltpu.VMEM((levels - 1, tiles, depth, depth), jnp.bfloat16),
            pltpu.VMEM((moves, rows, width, depth), jnp.bfloat16),
            pltpu.VMEM((moves, floors, width, depth), jnp.bfloat16),
            pltpu.VMEM((moves, floors, width, depth), jnp.bfloat16),
            pltpu.VMEM((moves, floors, width, depth), jnp.bfloat16),
            pltpu.VMEM((moves, floors, width, depth), jnp.bfloat16),
            pltpu.VMEM((moves, floors, width, depth), jnp.bfloat16),
            pltpu.VMEM((rows + 1, width, depth), jnp.bfloat16),
            pltpu.VMEM((tiles + 1, width, depth), jnp.bfloat16),
            pltpu.VMEM((width, depth), jnp.float32),
            dma((2,)),
            dma((1,)),
            dma((levels - 1,)),
            dma((moves,)),
            dma((moves,)),
            dma((moves,)),
            dma((moves,)),
            dma((moves,)),
            dma((moves,)),
        ],
        compiler_params=pltpu.CompilerParams(
            collective_id=0, has_side_effects=True, vmem_limit_bytes=VMEM_LIMIT
        ),
        name="level_solve",
    )(tile_source[:, 0], tile_target[:, 0], right_side[0, 0], diag_inverse[0, 0], panels[:, 0])
    solved = jnp.swapaxes(solved.reshape(levels, cols, depth), 1, 2)
    return solved[None, None]


def solution(mesh):
    return jax.shard_map(
        functools.partial(local, mesh.shape["row"], mesh.shape["col"]),
        mesh=mesh,
        in_specs=(
            P("row", "col", None, None, None),
            P("row", "col", None, None, None),
            P(None, "row", "col", None, None),
            P(None, "row", "col"),
            P(None, "row", "col"),
        ),
        out_specs=P("row", "col", None, None, None),
        check_vma=False,
    )
```

```python
import functools
import math

import jax
import jax.numpy as jnp
from jax import lax
from jax.experimental import pallas as pl
from jax.experimental.pallas import tpu as pltpu
from jax.sharding import PartitionSpec as P

MESH = pl.DeviceIdType.MESH
CORES = 2
CHUNKS = 8
LISTS = 4
LATE_PRODUCT = 3
LATE_EXCHANGE = 4
NT = (((1,), (1,)), ((), ()))
VMEM_LIMIT = 60 * 1024 * 1024


def ordered_tiles(source, target, rows, columns, tiles):
    lanes = source.shape[1]
    key = (target * lanes + lax.broadcasted_iota(jnp.int32, source.shape, 1)) * rows + source
    across = jnp.broadcast_to(key, (lanes, lanes))
    down = across.T
    place = jnp.sum((down < across).astype(jnp.int32), axis=0, keepdims=True)
    slot = lax.broadcasted_iota(jnp.int32, (lanes, lanes), 1)
    placed = jnp.broadcast_to(place, (lanes, lanes)).T == slot
    ordered = jnp.sum(jnp.where(placed, down, 0), axis=0, keepdims=True)
    ends = jnp.sum((down < (slot + 1) * (lanes * rows)).astype(jnp.int32), axis=0, keepdims=True)
    number = ordered // rows
    return [
        jnp.clip(lax.rem(number, lanes), 0, tiles - 1),
        jnp.clip(lax.rem(ordered, rows), 0, rows - 1),
        number // lanes,
        jnp.clip(ends, 0, tiles),
    ]


def torus_order(rows):
    side = math.isqrt(rows)
    steps = [(dx, dy) for dx in range(side) for dy in range(side) if dx or dy]

    def far(step):
        return -sum(min(part, side - part) for part in step)

    return side, sorted(steps, key=far)


def ring_order(length):
    return sorted(range(1, length), key=lambda step: -min(step, length - step))


def kernel(
    rows, columns, levels, chunks, tiles,
    source_hbm, target_hbm, rhs_hbm, diag_hbm, panels_hbm, out_hbm,
    source_ids, target_ids, out, straight, table, lists, source_pad, target_pad, right, rhs, diag, panels, gathered, given, kept, traded, passed, arrived, work, runs, current,
    out_sem, load_sem, table_sem, panel_sem, gather_send, gather_recv, trade_send, trade_recv, pass_send, pass_recv,
):
    me_row, me_col = lax.axis_index("row"), lax.axis_index("col")
    floors = columns // CORES
    floor, core = me_col // CORES, lax.rem(me_col, CORES)
    side, row_steps = torus_order(rows)
    me_x, me_y = me_row // side, lax.rem(me_row, side)
    moves = (levels - 1) * chunks
    width, depth = rhs.shape[1:]

    def row_peer(step):
        return lax.rem(me_x + step[0], side) * side + lax.rem(me_y + step[1], side)

    def floor_peer(step):
        return lax.rem(floor + step, floors)

    partner = floor * CORES + 1 - core

    loads = [
        pltpu.make_async_copy(rhs_hbm, right, load_sem.at[0]),
        pltpu.make_async_copy(diag_hbm, diag, load_sem.at[1]),
    ]
    id_loads = [
        pltpu.make_async_copy(source_hbm, source_ids, load_sem.at[2]),
        pltpu.make_async_copy(target_hbm, target_ids, load_sem.at[3]),
    ]
    panel_loads = [
        pltpu.make_async_copy(panels_hbm.at[level], panels.at[level], panel_sem.at[level])
        for level in range(levels - 1)
    ]
    for load in loads + id_loads + panel_loads:
        load.start()

    barrier = pltpu.get_barrier_semaphore()
    for step in row_steps:
        pl.semaphore_signal(barrier, inc=1, device_id=(row_peer(step), me_col), device_id_type=MESH)
    for step in ring_order(floors):
        pl.semaphore_signal(
            barrier, inc=1, device_id=(me_row, floor_peer(step) * CORES + core), device_id_type=MESH
        )
    pl.semaphore_signal(barrier, inc=1, device_id=(me_row, partner), device_id_type=MESH)

    work[rows] = jnp.zeros_like(work[rows])
    runs[tiles] = jnp.zeros_like(runs[tiles])
    for load in loads:
        load.wait()
    with jax.named_scope("wait_barrier"):
        pl.semaphore_wait(barrier, rows - 1 + floors - 1 + 1)

    def leave(level):
        return pltpu.make_async_copy(straight.at[level], out_hbm.at[level], out_sem.at[level])

    def finish(level):
        block = out[pl.ds(level * chunks, chunks)].reshape(chunks * width, depth)
        straight[level] = block.T
        leave(level).start()

    def turned(level):
        block = right[level].astype(jnp.float32).T
        rhs[pl.ds(level * chunks, chunks)] = block.reshape(chunks, width, depth)

    def plan():
        target_pad[...] = jnp.full_like(target_pad, columns)
        source_pad[...] = jnp.zeros_like(source_pad)
        for load in id_loads:
            load.wait()
        for level in range(levels - 1):
            target_pad[pl.ds(level, 1), pl.ds(0, tiles)] = target_ids[level]
            source_pad[pl.ds(level, 1), pl.ds(0, tiles)] = source_ids[level]
        for level in range(levels - 1):
            found = ordered_tiles(
                source_pad[pl.ds(level, 1)], target_pad[pl.ds(level, 1)], rows, columns, tiles
            )
            for place, values in enumerate(found):
                lists[pl.ds(LISTS * level + place, 1)] = values
        copy = pltpu.make_async_copy(lists, table, table_sem.at[0])
        copy.start()
        for level in range(1, levels):
            turned(level)
        copy.wait()

    def landed(ref, sem):
        pltpu.make_async_copy(ref, ref, sem).wait()

    def solve(g):
        level = g // chunks
        current[...] = rhs[g]

        @pl.when(g >= chunks)
        def _():
            h = g - chunks
            with jax.named_scope("wait_pass"):
                landed(arrived.at[h, pl.ds(0, floors - 1)], pass_recv.at[h])
            incoming = arrived[h, 0].astype(jnp.float32)
            for z in range(1, floors):
                incoming = incoming + arrived[h, z].astype(jnp.float32)
            current[...] = current[...] - incoming

        block = lax.dot_general(
            current[...].astype(jnp.bfloat16), diag[level],
            NT, preferred_element_type=jnp.float32,
        )

        @pl.when(g < moves)
        def _():
            gathered[g, me_row] = block.astype(jnp.bfloat16)
            for step in row_steps:
                pltpu.make_async_remote_copy(
                    src_ref=gathered.at[g, me_row],
                    dst_ref=gathered.at[g, me_row],
                    send_sem=gather_send.at[g],
                    recv_sem=gather_recv.at[g],
                    device_id=(row_peer(step), me_col),
                    device_id_type=MESH,
                ).start()

        out[g] = block

    def multiply(h):
        level = h // chunks

        @pl.when(h == 0)
        def _():
            for load in panel_loads:
                load.wait()

        with jax.named_scope("wait_gather"):
            landed(gathered.at[h, pl.ds(0, rows - 1)], gather_recv.at[h])
        for row in range(rows):
            work[row] = gathered[h, row]
        nothing = jnp.zeros((width, depth), jnp.bfloat16)
        total = jnp.zeros((width, depth), jnp.float32)
        before = -1
        for first in range(0, tiles, 2):
            second = first + 1
            tile = panels[level, table[LISTS * level, first]]
            block = work[table[LISTS * level + 1, first]]
            target = table[LISTS * level + 2, first]
            if second == tiles:
                product = lax.dot_general(block, tile, NT, preferred_element_type=jnp.float32)
                runs[first] = (product + jnp.where(target == before, total, 0.0)).astype(jnp.bfloat16)
                break
            tile = jnp.concatenate([tile, panels[level, table[LISTS * level, second]]], axis=1)
            source = table[LISTS * level + 1, second]
            same = table[LISTS * level + 2, second] == target
            picked = jnp.concatenate(
                [
                    jnp.concatenate([block, work[jnp.where(same, source, rows)]], axis=1),
                    jnp.concatenate([nothing, work[jnp.where(same, rows, source)]], axis=1),
                ],
                axis=0,
            )
            product = lax.dot_general(picked, tile, NT, preferred_element_type=jnp.float32)
            total = product[:width] + jnp.where(target == before, total, 0.0)
            runs[first] = total.astype(jnp.bfloat16)
            total = jnp.where(same, total, product[width:])
            runs[second] = total.astype(jnp.bfloat16)
            before = table[LISTS * level + 2, second]

        def summed(column):
            end = table[LISTS * level + 3, column]
            start = jnp.where(column == 0, 0, table[LISTS * level + 3, jnp.maximum(column - 1, 0)])
            return runs[jnp.where(end > start, end - 1, tiles)]

        for z in range(floors):
            given[h, z] = summed(CORES * z + 1 - core)
        pltpu.make_async_remote_copy(
            src_ref=given.at[h],
            dst_ref=traded.at[h],
            send_sem=trade_send.at[h],
            recv_sem=trade_recv.at[h],
            device_id=(me_row, partner),
            device_id_type=MESH,
        ).start()
        for z in range(floors):
            kept[h, z] = summed(CORES * z + core)

    def exchange(h):
        with jax.named_scope("wait_trade"):
            landed(traded.at[h], trade_recv.at[h])

        def both(z):
            return (kept[h, z].astype(jnp.float32) + traded[h, z].astype(jnp.float32)).astype(jnp.bfloat16)

        for step in ring_order(floors):
            z = floor_peer(step)
            passed[h, z] = both(z)
            pltpu.make_async_remote_copy(
                src_ref=passed.at[h, z],
                dst_ref=arrived.at[h, floor],
                send_sem=pass_send.at[h],
                recv_sem=pass_recv.at[h],
                device_id=(me_row, z * CORES + core),
                device_id_type=MESH,
            ).start()
        arrived[h, floor] = both(floor)

    def stage(run, h):
        @pl.when((h >= 0) & (h < moves))
        def _():
            with jax.named_scope(run.__name__):
                run(h)

    def turn(g, carry):
        @pl.when(g > LATE_PRODUCT)
        def _():
            with jax.named_scope("solve"):
                solve(g)

        stage(multiply, g - LATE_PRODUCT)
        stage(exchange, g - LATE_EXCHANGE)

        @pl.when(lax.rem(g, chunks) == chunks - 1)
        def _():
            with jax.named_scope("finish"):
                finish(g // chunks)

        return carry

    def begin(g, carry):
        solve(g)
        return carry

    turned(0)
    lax.fori_loop(0, LATE_PRODUCT + 1, begin, 0)
    with jax.named_scope("plan"):
        plan()
    lax.fori_loop(0, levels * chunks, turn, 0)

    def drain(h, carry):
        landed(gathered.at[h, pl.ds(0, rows - 1)], gather_send.at[h])
        landed(given.at[h], trade_send.at[h])
        landed(passed.at[h, pl.ds(0, floors - 1)], pass_send.at[h])
        return carry

    lax.fori_loop(0, moves, drain, 0)
    for level in range(levels):
        leave(level).wait()


def local(rows, columns, right_side, diag_inverse, panels, tile_source, tile_target):
    levels, depth, cols = right_side.shape[2:]
    tiles = panels.shape[2]
    chunks = CHUNKS
    width = cols // chunks
    moves = (levels - 1) * chunks
    floors = columns // CORES
    lanes = -(-tiles // depth) * depth
    dma = pltpu.SemaphoreType.DMA
    anywhere = pl.BlockSpec(memory_space=pl.ANY)
    solved = pl.pallas_call(
        functools.partial(kernel, rows, columns, levels, chunks, tiles),
        out_shape=jax.ShapeDtypeStruct((levels, depth, cols), jnp.float32),
        in_specs=[anywhere] * 5,
        out_specs=anywhere,
        scratch_shapes=[
            pltpu.VMEM((levels - 1, 1, tiles), jnp.int32),
            pltpu.VMEM((levels - 1, 1, tiles), jnp.int32),
            pltpu.VMEM((levels * chunks, width, depth), jnp.float32),
            pltpu.VMEM((levels, depth, cols), jnp.float32),
            pltpu.SMEM((LISTS * levels, lanes), jnp.int32),
            pltpu.VMEM((LISTS * levels, lanes), jnp.int32),
            pltpu.VMEM((levels, lanes), jnp.int32),
            pltpu.VMEM((levels, lanes), jnp.int32),
            pltpu.VMEM((levels, depth, cols), jnp.bfloat16),
            pltpu.VMEM((levels * chunks, width, depth), jnp.float32),
            pltpu.VMEM((levels, depth, depth), jnp.bfloat16),
            pltpu.VMEM((levels - 1, tiles, depth, depth), jnp.bfloat16),
            pltpu.VMEM((moves, rows, width, depth), jnp.bfloat16),
            pltpu.VMEM((moves, floors, width, depth), jnp.bfloat16),
            pltpu.VMEM((moves, floors, width, depth), jnp.bfloat16),
            pltpu.VMEM((moves, floors, width, depth), jnp.bfloat16),
            pltpu.VMEM((moves, floors, width, depth), jnp.bfloat16),
            pltpu.VMEM((moves, floors, width, depth), jnp.bfloat16),
            pltpu.VMEM((rows + 1, width, depth), jnp.bfloat16),
            pltpu.VMEM((tiles + 1, width, depth), jnp.bfloat16),
            pltpu.VMEM((width, depth), jnp.float32),
            dma((levels,)),
            dma((4,)),
            dma((1,)),
            dma((levels - 1,)),
            dma((moves,)),
            dma((moves,)),
            dma((moves,)),
            dma((moves,)),
            dma((moves,)),
            dma((moves,)),
        ],
        compiler_params=pltpu.CompilerParams(
            collective_id=0, has_side_effects=True, vmem_limit_bytes=VMEM_LIMIT
        ),
        name="level_solve",
    )(tile_source, tile_target, right_side[0, 0], diag_inverse[0, 0], panels[:, 0])
    return solved[None, None]


def solution(mesh):
    return jax.shard_map(
        functools.partial(local, mesh.shape["row"], mesh.shape["col"]),
        mesh=mesh,
        in_specs=(
            P("row", "col", None, None, None),
            P("row", "col", None, None, None),
            P(None, "row", "col", None, None),
            P(None, "row", "col"),
            P(None, "row", "col"),
        ),
        out_specs=P("row", "col", None, None, None),
        check_vma=False,
    )
```
